16 devices in a mesh: rep: 1, dp: 16 (over x, y, z, core).
Axes of the slice: x: 2, y: 2, z: 2, core: 2. Of those that a mesh axis runs over, the one named last changes fastest.
Arguments:
- x: bfloat16 [16, 2048, 512], P(('rep', 'dp'))
- dy: bfloat16 [16, 2048, 512], P(('rep', 'dp'))
- wq: bfloat16 [2, 512, 2048], replicated
- wk: bfloat16 [2, 512, 2048], replicated
- wv: bfloat16 [2, 512, 2048], replicated
- wo: bfloat16 [2, 2048, 512], replicated
- w_gate: bfloat16 [2, 512, 8192], replicated
- w_up: bfloat16 [2, 512, 8192], replicated
- w_down: bfloat16 [2, 8192, 512], replicated
- m_wq: float32 [2, 512, 2048], P(None, 'dp')
- m_wk: float32 [2, 512, 2048], P(None, 'dp')
- m_wv: float32 [2, 512, 2048], P(None, 'dp')
- m_wo: float32 [2, 2048, 512], P(None, 'dp')
- m_w_gate: float32 [2, 512, 8192], P(None, 'dp')
- m_w_up: float32 [2, 512, 8192], P(None, 'dp')
- m_w_down: float32 [2, 8192, 512], P(None, 'dp')
- v_wq: float32 [2, 512, 2048], P(None, 'dp')
- v_wk: float32 [2, 512, 2048], P(None, 'dp')
- v_wv: float32 [2, 512, 2048], P(None, 'dp')
- v_wo: float32 [2, 2048, 512], P(None, 'dp')
- v_w_gate: float32 [2, 512, 8192], P(None, 'dp')
- v_w_up: float32 [2, 512, 8192], P(None, 'dp')
- v_w_down: float32 [2, 8192, 512], P(None, 'dp')
Outputs:
- output 1: bfloat16 [2, 512, 2048], P('rep')
- output 2: bfloat16 [2, 512, 2048], P('rep')
- output 3: bfloat16 [2, 512, 2048], P('rep')
- output 4: bfloat16 [2, 2048, 512], P('rep')
- output 5: bfloat16 [2, 512, 8192], P('rep')
- output 6: bfloat16 [2, 512, 8192], P('rep')
- output 7: bfloat16 [2, 8192, 512], P('rep')
- output 8: float32 [2, 512, 2048], P('rep', 'dp')
- output 9: float32 [2, 512, 2048], P('rep', 'dp')
- output 10: float32 [2, 512, 2048], P('rep', 'dp')
- output 11: float32 [2, 2048, 512], P('rep', 'dp')
- output 12: float32 [2, 512, 8192], P('rep', 'dp')
- output 13: float32 [2, 512, 8192], P('rep', 'dp')
- output 14: float32 [2, 8192, 512], P('rep', 'dp')
- output 15: float32 [2, 512, 2048], P('rep', 'dp')
- output 16: float32 [2, 512, 2048], P('rep', 'dp')
- output 17: float32 [2, 512, 2048], P('rep', 'dp')
- output 18: float32 [2, 2048, 512], P('rep', 'dp')
- output 19: float32 [2, 512, 8192], P('rep', 'dp')
- output 20: float32 [2, 512, 8192], P('rep', 'dp')
- output 21: float32 [2, 8192, 512], P('rep', 'dp')
All inputs are finite; a program needn't handle non-finite values.
Results may differ from the reference program's by a relative error of at most 0.0252.
Values are sent between devices in bfloat16 or wider.
A program may use at most 2 GiB of HBM per device.

```python
import jax
import jax.numpy as jnp
from jax import lax

SEQUENCES = 16
TOKENS = 2048
D = 512
HEADS = 16
KV_HEADS = 16
HEAD = 128
FF = 8192
LAYERS = 2
THETA = 10000
NAMES = ("wq", "wk", "wv", "wo", "w_gate", "w_up", "w_down")
SHAPES = {
    "wq": (LAYERS, D, HEADS * HEAD),
    "wk": (LAYERS, D, KV_HEADS * HEAD),
    "wv": (LAYERS, D, KV_HEADS * HEAD),
    "wo": (LAYERS, HEADS * HEAD, D),
    "w_gate": (LAYERS, D, FF),
    "w_up": (LAYERS, D, FF),
    "w_down": (LAYERS, FF, D),
}


def bump(key, n, height):
    away = (jnp.arange(n, dtype=jnp.int32) - jax.random.randint(key, (), 0, n, jnp.int32)) % n
    return jnp.where(away < n // 8, height, 1.0)


def together(key, own, strength):
    shared = jax.random.normal(key, own.shape[1:], jnp.float32)
    return (own + strength * shared) * lax.rsqrt(1 + strength * strength)


def setup_inputs(seed: int = 0, part: int = 0) -> dict:
    kx, kdy, ka, kb, kz, kf, kh, kl, *keys = jax.random.split(jax.random.key(seed), 8 + 3 * len(NAMES))
    kx, kdy, ka, kb = (jax.random.fold_in(k, part) for k in (kx, kdy, ka, kb))
    kw, km, kv = (keys[i::3] for i in range(3))
    shape = (SEQUENCES, TOKENS, D)
    much_x, much_dy = jax.random.uniform(kz, (2,), jnp.float32, 0.0, 1.0)
    loud = 2.0 ** jax.random.uniform(jax.random.fold_in(kz, 1), (), jnp.float32, -1.0, 2.0)
    layers = 2.0 ** jax.random.uniform(kl, (LAYERS, 1, 1), jnp.float32, -1.0, 1.0)
    times = {"wq": 1.0, "wk": 1.0, "wv": 2.0, "wo": layers, "w_gate": 1.0, "w_up": bump(kh, FF, 4.0), "w_down": layers}
    x = together(ka, jax.random.normal(kx, shape, jnp.float32), much_x) * bump(kf, D, 4.0)
    dy = together(kb, jax.random.normal(kdy, shape, jnp.float32), much_dy)
    drawn = {"x": x.astype(jnp.bfloat16), "dy": (loud * dy * (SEQUENCES * TOKENS) ** -0.5).astype(jnp.bfloat16)}
    for key, name in zip(kw, NAMES, strict=True):
        drawn[name] = (jax.random.normal(key, SHAPES[name], jnp.float32) * SHAPES[name][1] ** -0.5 * times[name]).astype(jnp.bfloat16)
    for key, name in zip(km, NAMES, strict=True):
        drawn[f"m_{name}"] = 0.1 * jax.random.normal(key, SHAPES[name], jnp.float32)
    for key, name in zip(kv, NAMES, strict=True):
        drawn[f"v_{name}"] = jax.random.uniform(key, SHAPES[name], jnp.float32, 0.02, 0.06)
    return drawn


def matmul(a, w):
    return jnp.dot(a, w, preferred_element_type=jnp.float32).astype(jnp.bfloat16)


def normed(h):
    wide = h.astype(jnp.float32)
    scale = lax.rsqrt(jnp.mean(wide**2, -1, keepdims=True) + 1e-6)
    return (wide * scale).astype(jnp.bfloat16)


def turned(t, theta):
    half = t.shape[-1] // 2
    angle = jnp.arange(t.shape[0], dtype=jnp.float32)[:, None] * theta ** (-jnp.arange(half, dtype=jnp.float32) / half)
    cos, sin = jnp.cos(angle)[:, None], jnp.sin(angle)[:, None]
    a, b = t[..., :half].astype(jnp.float32), t[..., half:].astype(jnp.float32)
    return jnp.concatenate([a * cos - b * sin, b * cos + a * sin], -1).astype(jnp.bfloat16)


def seen_by(q, k, v):
    tokens, kv = q.shape[0], k.shape[1]
    q = q.reshape(tokens, kv, -1, q.shape[-1])
    scores = jnp.einsum("tgsd,ugd->gstu", q.astype(jnp.float32), k.astype(jnp.float32)) * q.shape[-1] ** -0.5
    place = jnp.arange(tokens)
    weights = jax.nn.softmax(jnp.where(place[:, None] >= place, scores, -jnp.inf), -1).astype(jnp.bfloat16)
    return jnp.einsum("gstu,ugd->tgsd", weights.astype(jnp.float32), v.astype(jnp.float32)).astype(jnp.bfloat16).reshape(tokens, -1)


def layer(h, w):
    a = normed(h)
    q, k = (turned(matmul(a, w[name]).reshape(h.shape[0], -1, HEAD), THETA) for name in ("wq", "wk"))
    h = h + matmul(seen_by(q, k, matmul(a, w["wv"]).reshape(h.shape[0], -1, HEAD)), w["wo"])
    b = normed(h)
    gate = jnp.dot(b, w["w_gate"], preferred_element_type=jnp.float32)
    up = jnp.dot(b, w["w_up"], preferred_element_type=jnp.float32)
    return h + matmul((jax.nn.silu(gate) * up).astype(jnp.bfloat16), w["w_down"])


def adamw(w, m, v, g):
    m = 0.9 * m + 0.1 * g
    v = 0.95 * v + 0.05 * g * g
    step = m * lax.rsqrt(v + 1e-8) + 0.1 * w
    return (w - 0.02 * step).astype(jnp.bfloat16), m, v


def clipped(gradients, sum_of_squares, count):
    factor = jnp.minimum(1.0, 0.5 * lax.rsqrt(sum_of_squares / count + 1e-30))
    return [g * factor for g in gradients]


def stack(weights, h):
    return lax.scan(lambda h, w: (layer(h, w), None), h, weights)[0]


def reference(x, dy, wq, wk, wv, wo, w_gate, w_up, w_down, m_wq, m_wk, m_wv, m_wo, m_w_gate, m_w_up, m_w_down, v_wq, v_wk, v_wv, v_wo, v_w_gate, v_w_up, v_w_down):
    weights = dict(zip(NAMES, (wq, wk, wv, wo, w_gate, w_up, w_down), strict=True))

    def take(so_far, sequence):
        h, by_y = sequence
        _, back = jax.vjp(stack, weights, h)
        by_weights, by_h = back(by_y)
        return jax.tree.map(lambda total, term: total + term.astype(jnp.float32), so_far, by_weights), by_h

    none_yet = {name: jnp.zeros(w.shape, jnp.float32) for name, w in weights.items()}
    by_weights, by_x = lax.scan(take, none_yet, (x, dy))
    gradients = [by_weights[name].astype(jnp.bfloat16).astype(jnp.float32) for name in NAMES]
    gradients = clipped(gradients, sum(jnp.sum(g * g) for g in gradients), sum(g.size for g in gradients))
    first = (m_wq, m_wk, m_wv, m_wo, m_w_gate, m_w_up, m_w_down)
    second = (v_wq, v_wk, v_wv, v_wo, v_w_gate, v_w_up, v_w_down)
    new = [adamw(weights[name].astype(jnp.float32), m, v, g) for name, m, v, g in zip(NAMES, first, second, gradients, strict=True)]
    return tuple(one[which] for which in range(3) for one in new)
```

```python
import functools

import jax
import jax.numpy as jnp
from jax import lax
from jax.experimental import pallas as pl
from jax.experimental.pallas import tpu as pltpu
from jax.sharding import PartitionSpec as P

HEAD = 128
THETA = 10000
NEG = -1e30
HIDDEN = 2 * NEG
LOG2E = 1.4426950408889634
VMEM = 60 * 2**20
BF, F32 = jnp.bfloat16, jnp.float32


def _dot(a, b, ca, cb):
    return lax.dot_general(a, b, (((ca,), (cb,)), ((), ())), preferred_element_type=F32)


def _call(kernel, grid, in_specs, out_specs, out_shape, scratch, flops, read, **more):
    return pl.pallas_call(
        kernel,
        grid_spec=pltpu.PrefetchScalarGridSpec(num_scalar_prefetch=0, grid=grid, in_specs=in_specs, out_specs=out_specs, scratch_shapes=scratch),
        out_shape=out_shape,
        compiler_params=pltpu.CompilerParams(dimension_semantics=("arbitrary",) * len(grid), vmem_limit_bytes=VMEM, **more),
        cost_estimate=pl.CostEstimate(flops=int(flops), transcendentals=0, bytes_accessed=int(read)),
    )


def _kept(shape):
    return pl.BlockSpec(shape, lambda *_: (0,) * len(shape), pipeline_mode=pl.Buffered(1))


def normed(h):
    wide = h.astype(F32)
    scale = lax.rsqrt(jnp.mean(wide**2, -1, keepdims=True) + 1e-6)
    return (wide * scale).astype(BF)


def tables(tokens):
    half = HEAD // 2
    angle = jnp.arange(tokens, dtype=F32)[:, None] * THETA ** (-jnp.arange(half, dtype=F32) / half)
    cos, sin = jnp.cos(angle), jnp.sin(angle)
    return jnp.concatenate([cos, cos], -1), jnp.concatenate([-sin, sin], -1)


def _turn(t, cos, sin):
    wide = t.astype(F32)
    return (wide * cos + pltpu.roll(wide, HEAD // 2, 1) * sin).astype(BF)


def _qkv_kernel(h_ref, wq_ref, wk_ref, wv_ref, cos_ref, sin_ref, a_ref, q_ref, k_ref, v_ref):
    a = normed(h_ref[...])
    a_ref[...] = a
    cos, sin = cos_ref[...], sin_ref[...]
    for w_ref, o_ref, turns in ((wq_ref, q_ref, True), (wk_ref, k_ref, True), (wv_ref, v_ref, False)):
        for n in range(0, o_ref.shape[1], 512):
            t = _dot(a, w_ref[0, :, n : n + 512], 1, 0).astype(BF)
            for at in range(0, 512, HEAD):
                one = t[:, at : at + HEAD]
                o_ref[:, n + at : n + at + HEAD] = _turn(one, cos, sin) if turns else one


def qkv(h, wq, wk, wv, cos, sin, number):
    tokens, d = h.shape
    wide = wq.shape[2]
    bt = 256
    rows = lambda n: pl.BlockSpec((bt, n), lambda i: (i, 0))
    weight = pl.BlockSpec((1, d, wide), lambda i: (number, 0, 0), pipeline_mode=pl.Buffered(1))
    return _call(_qkv_kernel, (tokens // bt,), [rows(d), weight, weight, weight, rows(HEAD), rows(HEAD)], [rows(d)] + [rows(wide)] * 3,
                 [jax.ShapeDtypeStruct((tokens, d), BF)] + [jax.ShapeDtypeStruct((tokens, wide), BF)] * 3, [],
                 6 * tokens * d * wide, 6 * d * wide + 6 * tokens * wide)(h, wq, wk, wv, cos, sin)


def _gap(bk, cols):
    return lax.broadcasted_iota(jnp.int32, (bk, cols), 1) - lax.broadcasted_iota(jnp.int32, (bk, cols), 0)


def _attend_kernel(q_ref, k_ref, v_ref, o_ref, lse_ref, top_s, mix_s, gap_s, *, scale, bq, bk, heads):
    iq = pl.program_id(0)
    e = scale * LOG2E

    @pl.when(iq == 0)
    def _():
        gap_s[...] = _gap(bq, bq)

    top_s[...] = jnp.full(top_s.shape, NEG, F32)
    mix_s[...] = jnp.zeros(mix_s.shape, F32)
    ones = jnp.ones((8, bk), BF)
    cut = [slice(i * HEAD, (i + 1) * HEAD) for i in range(heads)]

    def block(start, size, masked):
        here = pl.ds(pl.multiple_of(start, size), size)
        scores = [_dot(k_ref[here, c], q_ref[:, c], 1, 1) for c in cut]
        ok = gap_s[...] >= 0 if masked else None
        weights, keeps = [], []
        for i, s in enumerate(scores):
            if masked:
                s = jnp.where(ok, s, HIDDEN)
            old = top_s[i : i + 1, :]
            top = jnp.maximum(old, s.max(axis=0, keepdims=True))
            top_s[i : i + 1, :] = top
            weights.append(jnp.exp2((s - top) * e).astype(BF))
            keeps.append(jnp.exp2((old - top) * e))
        for i, (p, keep) in enumerate(zip(weights, keeps)):
            values = jnp.concatenate([v_ref[here, cut[i]].T, ones[:, :size]], axis=0)
            mix_s[i] = mix_s[i] * keep + _dot(values, p, 1, 0)

    whole = lax.div(iq * bq, bk)
    lax.fori_loop(0, whole, lambda j, _: block(j * bk, bk, False), None)

    @pl.when(lax.rem(iq, 2) == 1)
    def _():
        block((iq - 1) * bq, bq, False)

    block(iq * bq, bq, True)
    for i in range(heads):
        top, total = top_s[i : i + 1, :], mix_s[i, HEAD : HEAD + 1, :]
        o_ref[:, cut[i]] = (mix_s[i, :HEAD, :] * (1 / total)).T.astype(BF)
        lse_ref[i : i + 1, :] = top * scale + jnp.log(total)


def attend(q, k, v):
    tokens, wide = q.shape
    heads = wide // HEAD
    bq, bk = 256, 512
    rows = pl.BlockSpec((bq, wide), lambda i: (i, 0))
    kernel = functools.partial(_attend_kernel, scale=HEAD**-0.5, bq=bq, bk=bk, heads=heads)
    return _call(kernel, (tokens // bq,), [rows, _kept((tokens, wide)), _kept((tokens, wide))],
                 [rows, pl.BlockSpec((heads, bq), lambda i: (0, i))],
                 [jax.ShapeDtypeStruct((tokens, wide), BF), jax.ShapeDtypeStruct((heads, tokens), F32)],
                 [pltpu.VMEM((heads, bq), F32), pltpu.VMEM((heads, HEAD + 8, bq), F32), pltpu.VMEM((bq, bq), jnp.int32)],
                 4 * tokens * tokens * wide, 8 * tokens * wide)(q, k, v)


def _attend_bwd_kernel(q_ref, k_ref, v_ref, do_ref, o_ref, lse_ref, cos_ref, sin_ref, dq_ref, dk_ref, dv_ref, dq_s, dk_s, dv_s, gap_s,
                       *, scale, bq, bk, heads):
    iq = pl.program_id(1)
    e = scale * LOG2E
    cut = [slice(i * HEAD, (i + 1) * HEAD) for i in range(heads)]

    @pl.when(iq == 0)
    def _():
        gap_s[...] = _gap(bq // 2, bq)
        dk_s[...] = jnp.zeros_like(dk_s)
        dv_s[...] = jnp.zeros_like(dv_s)

    dq_s[...] = jnp.zeros_like(dq_s)
    lses = [lse_ref[0, i : i + 1, :] * LOG2E for i in range(heads)]
    row = jnp.ones((8, HEAD), BF)
    deltas = []
    for c in cut:
        both = do_ref[:, c].astype(F32) * o_ref[:, c].astype(F32)
        high = both.astype(BF)
        low = (both - high.astype(F32)).astype(BF)
        deltas.append((_dot(row, high, 1, 1) + _dot(row, low, 1, 1))[:1, :])

    def block(start, size, first, masked):
        here = pl.ds(pl.multiple_of(start, size), size)
        qs, dos = [q_ref[first:, c] for c in cut], [do_ref[first:, c] for c in cut]
        scores = [_dot(k_ref[here, c], x, 1, 1) for c, x in zip(cut, qs)]
        dps = [_dot(v_ref[here, c], x, 1, 1) for c, x in zip(cut, dos)]
        ok = gap_s[:size, : bq - first] >= 0 if masked else None
        for i, c in enumerate(cut):
            p = jnp.exp2(scores[i] * e - lses[i][:, first:])
            if masked:
                p = jnp.where(ok, p, 0.0)
            ds = (p * (dps[i] - deltas[i][:, first:])).astype(BF)
            dv_s[i, here, :] += _dot(p.astype(BF), dos[i], 1, 0)
            dk_s[i, here, :] += _dot(ds, qs[i], 1, 0)
            dq_s[i, :, first:] += _dot(k_ref[here, c].T, ds, 1, 0)

    half = bq // 2
    lax.fori_loop(0, iq, lambda j, _: block(j * bk, bk, 0, False), None)
    block(iq * bq, half, 0, True)
    block(iq * bq + half, half, half, True)
    here = pl.ds(pl.multiple_of(iq * bq, bq), bq)
    for i, c in enumerate(cut):
        dq_ref[:, c] = _turn((dq_s[i] * scale).T.astype(BF), cos_ref[here, :], -sin_ref[here, :])

    @pl.when(iq == pl.num_programs(1) - 1)
    def _():
        for i, c in enumerate(cut):
            dk_ref[:, c] = _turn((dk_s[i] * scale).astype(BF), cos_ref[...], -sin_ref[...])
            dv_ref[:, c] = dv_s[i].astype(BF)


def attend_bwd(q, k, v, do, o, lse, cos, sin):
    tokens, wide = q.shape
    heads = 4
    groups = wide // HEAD // heads
    bq, bk = 512, 512
    rows = pl.BlockSpec((bq, heads * HEAD), lambda g, i: (i, g))
    keys = pl.BlockSpec((tokens, heads * HEAD), lambda g, i: (0, g))
    kernel = functools.partial(_attend_bwd_kernel, scale=HEAD**-0.5, bq=bq, bk=bk, heads=heads)
    return _call(kernel, (groups, tokens // bq),
                 [rows, keys, keys, rows, rows, pl.BlockSpec((1, heads, bq), lambda g, i: (g, 0, i)), _kept((tokens, HEAD)), _kept((tokens, HEAD))],
                 [rows, keys, keys], [jax.ShapeDtypeStruct((tokens, wide), BF)] * 3,
                 [pltpu.VMEM((heads, HEAD, bq), F32), pltpu.VMEM((heads, tokens, HEAD), F32), pltpu.VMEM((heads, tokens, HEAD), F32),
                  pltpu.VMEM((bq // 2, bq), jnp.int32)],
                 10 * tokens * tokens * wide, 16 * tokens * wide)(q, k, v, do, o, lse.reshape(groups, heads, tokens), cos, sin)


def _sigmoid(x):
    return 0.5 * jnp.tanh(0.5 * x) + 0.5


def _mlp_kernel(b_ref, h_ref, wg_ref, wu_ref, wd_ref, out_ref, acc_s, *, bt):
    j = pl.program_id(0)

    @pl.when(j == 0)
    def _():
        acc_s[...] = jnp.zeros_like(acc_s)

    for at in range(0, b_ref.shape[0], bt):
        b = b_ref[at : at + bt, :]
        gate, up = _dot(b, wg_ref[0], 1, 0), _dot(b, wu_ref[0], 1, 0)
        act = (gate * _sigmoid(gate) * up).astype(BF)
        acc_s[at : at + bt, :] += _dot(act, wd_ref[0], 1, 0)

    @pl.when(j == pl.num_programs(0) - 1)
    def _():
        out_ref[...] = h_ref[...] + acc_s[...].astype(BF)


def mlp(b, h, wg, wu, wd, number):
    tokens, d = b.shape
    ff = wg.shape[2]
    bf = 512
    across = pl.BlockSpec((1, d, bf), lambda j: (number, 0, j))
    down = pl.BlockSpec((1, bf, d), lambda j: (number, j, 0))
    whole = _kept((tokens, d))
    return _call(functools.partial(_mlp_kernel, bt=512), (ff // bf,), [whole, whole, across, across, down], whole,
                 jax.ShapeDtypeStruct((tokens, d), BF), [pltpu.VMEM((tokens, d), F32)],
                 6 * tokens * d * ff, 6 * d * ff)(b, h, wg, wu, wd)


def _mlp_bwd_kernel(b_ref, do_ref, wg_ref, wu_ref, wd_ref, db_ref, dw_ref, bt_s, dot_s, act_s, dg_s, du_s, dbt_s, stage, sems, *, bt):
    j, blocks = pl.program_id(0), pl.num_programs(0)
    tokens, _ = b_ref.shape
    slot = lax.rem(j, 2)

    @pl.when(j == 0)
    def _():
        for at in range(0, tokens, bt):
            bt_s[:, at : at + bt] = b_ref[at : at + bt, :].T
            dot_s[:, at : at + bt] = do_ref[at : at + bt, :].T
        dbt_s[...] = jnp.zeros_like(dbt_s)

    def copies(j, slot):
        targets = (dw_ref.at[:, j], dw_ref.at[:, blocks + j], dw_ref.at[j, pl.ds(2 * blocks, blocks)])
        return [pltpu.make_async_copy(stage.at[slot, n], to, sems.at[slot, n]) for n, to in enumerate(targets)]

    @pl.when(j >= 2)
    def _():
        for copy in copies(j - 2, slot):
            copy.wait()

    wg, wu, wd = wg_ref[0], wu_ref[0], wd_ref[0]
    wgt, wut = wg.T, wu.T
    for at in range(0, tokens, bt):
        b = bt_s[:, at : at + bt]
        gate, up = _dot(wgt, b, 1, 0), _dot(wut, b, 1, 0)
        da = _dot(wd, dot_s[:, at : at + bt], 1, 0).astype(BF).astype(F32)
        s = _sigmoid(gate)
        silu = gate * s
        act_s[:, at : at + bt] = (silu * up).astype(BF)
        du = (da * silu).astype(BF)
        dg = (da * up * (s + silu * (1 - s))).astype(BF)
        du_s[:, at : at + bt] = du
        dg_s[:, at : at + bt] = dg
        dbt_s[:, at : at + bt] += _dot(wg, dg, 1, 0) + _dot(wu, du, 1, 0)
    b, do = b_ref[...], do_ref[...]
    shape = stage.shape[2:]
    stage[slot, 0] = _dot(dg_s[...], b, 1, 0).astype(BF).T.reshape(shape)
    stage[slot, 1] = _dot(du_s[...], b, 1, 0).astype(BF).T.reshape(shape)
    stage[slot, 2] = _dot(act_s[...], do, 1, 0).astype(BF).reshape(shape)
    for copy in copies(j, slot):
        copy.start()

    @pl.when(j == blocks - 1)
    def _():
        for at in range(0, tokens, bt):
            db_ref[at : at + bt, :] = dbt_s[:, at : at + bt].T.astype(BF)
        for copy in copies(j - 1, 1 - slot):
            copy.wait()
        for copy in copies(j, slot):
            copy.wait()


def mlp_bwd(b, do, wg, wu, wd, number, parts):
    tokens, d = b.shape
    ff = wg.shape[2]
    bf = ff // parts
    rows = d // parts
    across = pl.BlockSpec((1, d, bf), lambda j: (number, 0, j))
    down = pl.BlockSpec((1, bf, d), lambda j: (number, j, 0))
    whole = _kept((tokens, d))
    return _call(functools.partial(_mlp_bwd_kernel, bt=512), (parts,), [whole, whole, across, across, down],
                 [whole, pl.BlockSpec(memory_space=pl.ANY)],
                 [jax.ShapeDtypeStruct((tokens, d), BF), jax.ShapeDtypeStruct((parts, 3 * parts, rows, d), BF)],
                 [pltpu.VMEM((d, tokens), BF), pltpu.VMEM((d, tokens), BF)] + [pltpu.VMEM((bf, tokens), BF)] * 3
                 + [pltpu.VMEM((d, tokens), F32), pltpu.VMEM((2, 3, parts, rows, d), BF), pltpu.SemaphoreType.DMA((2, 3))],
                 16 * tokens * d * ff, 12 * d * ff)(b, do, wg, wu, wd)


def _project_bwd_kernel(a_ref, dq_ref, dk_ref, dv_ref, wq_ref, wk_ref, wv_ref, dwo_ref, dw_ref, da_ref, at_s, da_s, *, per, onward):
    n = pl.program_id(0)
    tokens = a_ref.shape[0]

    @pl.when(n == 0)
    def _():
        for at in range(0, tokens, 512):
            at_s[:, at : at + 512] = a_ref[at : at + 512, :].T
        if onward:
            da_s[...] = jnp.zeros_like(da_s)

    for which, (g_ref, w_ref) in enumerate(((dq_ref, wq_ref), (dk_ref, wk_ref), (dv_ref, wv_ref))):
        @pl.when((n >= which * per) & (n < (which + 1) * per))
        def _(g_ref=g_ref, w_ref=w_ref):
            dw_ref[...] = _dot(at_s[...], g_ref[...], 1, 0).astype(BF).reshape(dw_ref.shape)
            if onward:
                for at in range(0, tokens, 512):
                    da_s[at : at + 512, :] += _dot(g_ref[at : at + 512, :], w_ref[0], 1, 1)

    @pl.when(n >= 3 * per)
    def _():
        dw_ref[...] = dwo_ref[...]

    @pl.when(n == pl.num_programs(0) - 1)
    def _():
        da_ref[...] = da_s[...].astype(BF) if onward else jnp.zeros_like(da_ref)


def project_bwd(a, dq, dk, dv, wq, wk, wv, dwo, number, parts, onward):
    tokens, d = a.shape
    wide = dq.shape[1]
    bc = 512
    per, rows = wide // bc, d // parts
    steps = 4 * per
    block = lambda which: lambda n: (0, jnp.clip(n - which * per, 0, per - 1))
    weight = lambda which: lambda n: (number, 0, jnp.clip(n - which * per, 0, per - 1))
    out_rows = (tokens, d) if onward else (8, d)
    return _call(functools.partial(_project_bwd_kernel, per=per, onward=onward), (steps,),
                 [_kept((tokens, d))] + [pl.BlockSpec((tokens, bc), block(i)) for i in range(3)] + [pl.BlockSpec((1, d, bc), weight(i)) for i in range(3)]
                 + [pl.BlockSpec((parts, 1, rows, d), lambda n: (0, jnp.clip(n - 3 * per, 0, per - 1), 0, 0))],
                 [pl.BlockSpec((parts, 1, rows, bc), lambda n: (0, n, 0, 0)), _kept(out_rows)],
                 [jax.ShapeDtypeStruct((parts, steps, rows, bc), BF), jax.ShapeDtypeStruct(out_rows, BF)],
                 [pltpu.VMEM((d, tokens), BF), pltpu.VMEM(out_rows, F32)],
                 (12 if onward else 6) * tokens * d * wide, 12 * tokens * wide)(
                     a, dq, dk, dv, wq, wk, wv, dwo.reshape(parts, per, rows, d))


def _total_kernel(x_ref, o_ref, slots, send, recv, *, n):
    me = lax.axis_index("dp")
    barrier = pltpu.get_barrier_semaphore()
    for k in range(1, n):
        pl.semaphore_signal(barrier, inc=1, device_id={"dp": lax.rem(me + k, n)}, device_id_type=pl.DeviceIdType.MESH)
    pl.semaphore_wait(barrier, n - 1)
    copies = []
    for k in range(1, n):
        copy = pltpu.make_async_remote_copy(src_ref=x_ref, dst_ref=slots.at[me], send_sem=send.at[k], recv_sem=recv.at[k],
                                            device_id={"dp": lax.rem(me + k, n)}, device_id_type=pl.DeviceIdType.MESH)
        copy.start()
        copies.append(copy)
    slots[me] = x_ref[...]
    for copy in copies:
        copy.wait()
    total = slots[0]
    for k in range(1, n):
        total = total + slots[k]
    o_ref[...] = total


def total(x, n):
    wide = jnp.broadcast_to(x, (8, 128))
    spec = pl.BlockSpec(memory_space=pltpu.VMEM)
    return pl.pallas_call(
        functools.partial(_total_kernel, n=n),
        out_shape=jax.ShapeDtypeStruct((8, 128), F32), in_specs=[spec], out_specs=spec,
        scratch_shapes=[pltpu.VMEM((n, 8, 128), F32), pltpu.SemaphoreType.DMA((n,)), pltpu.SemaphoreType.DMA((n,))],
        compiler_params=pltpu.CompilerParams(collective_id=0, has_side_effects=True), name="total",
    )(wide)[0, 0]


def matmul(a, w):
    return jnp.dot(a, w, preferred_element_type=F32).astype(BF)


def adamw(w, m, v, g):
    m = 0.9 * m + 0.1 * g
    v = 0.95 * v + 0.05 * g * g
    step = m * lax.rsqrt(v + 1e-8) + 0.1 * w
    return (w - 0.02 * step).astype(BF), m, v


def side_by_side(t):
    return t.transpose(1, 0, 2).reshape(t.shape[1], -1)


def solution(mesh):
    parts = mesh.shape["dp"]

    def work(x, dy, *arrays):
        weights, m, v = (arrays[i : i + 7] for i in (0, 7, 14))
        wq, wk, wv, wo, wg, wu, wd = weights
        layers, tokens = wq.shape[0], x.shape[1]
        cos, sin = tables(tokens)
        h, kept = x[0], []
        for n in range(layers):
            a, q, k, value = qkv(h, wq, wk, wv, cos, sin, n)
            o, lse = attend(q, k, value)
            mid = h + matmul(o, wo[n])
            b = normed(mid)
            kept.append((h, a, q, k, value, o, lse, mid, b))
            if n < layers - 1:
                h = mlp(b, mid, wg, wu, wd, n)
        by_h, mine = dy[0], [None] * layers
        for n in reversed(range(layers)):
            h, a, q, k, value, o, lse, mid, b = kept[n]
            by_b, dw = mlp_bwd(b, by_h, wg, wu, wd, n, parts)
            hidden = lax.psum_scatter(dw.reshape(parts, -1, dw.shape[-1]), "dp", scatter_dimension=0, tiled=True)[0]
            by_mid = by_h + jax.vjp(normed, mid)[1](by_b)[0]
            by_o, dwo = matmul(by_mid, wo[n].T), matmul(o.T, by_mid)
            dq, dk, dv = attend_bwd(q, k, value, by_o, o, lse, cos, sin)
            dw, by_a = project_bwd(a, dq, dk, dv, wq, wk, wv, dwo, n, parts, n > 0)
            heads = lax.psum_scatter(dw.reshape(parts, -1, dw.shape[-1]), "dp", scatter_dimension=0, tiled=True)[0]
            if n > 0:
                by_h = by_mid + jax.vjp(normed, h)[1](by_a)[0]
            rows = h.shape[1] // parts
            hidden, heads = (t.reshape(-1, rows, t.shape[-1]) for t in (hidden, heads))
            per = heads.shape[0] // 4
            mine[n] = [side_by_side(heads[i * per : (i + 1) * per]) for i in range(3)] + [heads[3 * per :].reshape(-1, h.shape[1])]
            mine[n] += [side_by_side(hidden[i * parts : (i + 1) * parts]) for i in range(2)] + [hidden[2 * parts :].reshape(-1, h.shape[1])]
        gradients = [jnp.stack([mine[n][i] for n in range(layers)]).astype(F32) for i in range(7)]
        squares = total(sum(jnp.sum(g * g) for g in gradients), parts)
        factor = jnp.minimum(1.0, 0.5 * lax.rsqrt(squares / (parts * sum(g.size for g in gradients)) + 1e-30))
        me = lax.axis_index("dp")
        own = [lax.dynamic_slice_in_dim(w, me * one.shape[1], one.shape[1], 1).astype(F32) for w, one in zip(weights, m, strict=True)]
        new = [adamw(w, m, v, g * factor) for w, m, v, g in zip(own, m, v, gradients, strict=True)]
        whole = gathered([one[0] for one in new], parts)
        return (*whole, *(one[1] for one in new), *(one[2] for one in new))

    states, all_of, cut = P(("rep", "dp"), None, None), P(None, None, None), P(None, "dp", None)
    return jax.shard_map(
        work,
        mesh=mesh,
        in_specs=(states, states) + (all_of,) * 7 + (cut,) * 14,
        out_specs=(P("rep", None, None),) * 7 + (P("rep", "dp", None),) * 14,
        check_vma=False,
    )


def _spread_kernel(*refs):
    count = len(refs) // 2
    for from_ref, to_ref in zip(refs[:count], refs[count:]):
        devices, _, rows, _ = from_ref.shape
        _, together, columns = to_ref.shape
        own = together // devices
        for n in range(devices):
            for at in range(0, own, rows):
                left = at // rows * columns
                to_ref[0, n * own + at : n * own + at + rows, :] = from_ref[n, 0, :, left : left + columns]


def spread(every, shapes, several):
    parts, slots, rows, columns = every.shape
    layers = slots // len(shapes)
    source = lambda at: pl.BlockSpec((several, 1, rows, columns), lambda n, i: (i, at * layers + n, 0, 0))
    target = lambda shape: pl.BlockSpec((1, several * shape[1] // parts, shape[2]), lambda n, i: (n, i, 0))
    return _call(_spread_kernel, (layers, parts // several), [source(at) for at in range(len(shapes))], [target(shape) for shape in shapes],
                 [jax.ShapeDtypeStruct(shape, BF) for shape in shapes], [], every.size, 4 * every.size)(*[every] * len(shapes))


def gathered(own, parts):
    out = [None] * 7
    for some, several in (((4, 5, 6), 1), ((0, 1, 2, 3), 4)):
        shape = own[some[0]].shape
        rows = shape[1]
        flat = [own[i].reshape(shape[0], -1, rows, own[i].shape[2]).transpose(0, 2, 1, 3).reshape(shape) for i in some]
        every = lax.all_gather(jnp.concatenate(flat, 0), "dp", axis=0)
        whole = spread(every, [(shape[0], own[i].shape[1] * parts, own[i].shape[2]) for i in some], several)
        for i, one in zip(some, whole):
            out[i] = one
    return out
```

```python
import functools

import jax
import jax.numpy as jnp
from jax import lax
from jax.experimental import pallas as pl
from jax.experimental.pallas import tpu as pltpu
from jax.sharding import PartitionSpec as P

HEAD = 128
THETA = 10000
NEG = -1e30
HIDDEN = 2 * NEG
LOG2E = 1.4426950408889634
VMEM = 60 * 2**20
BF, F32 = jnp.bfloat16, jnp.float32


def _dot(a, b, ca, cb):
    return lax.dot_general(a, b, (((ca,), (cb,)), ((), ())), preferred_element_type=F32)


def _call(kernel, grid, in_specs, out_specs, out_shape, scratch, flops, read, **more):
    return pl.pallas_call(
        kernel,
        grid_spec=pltpu.PrefetchScalarGridSpec(num_scalar_prefetch=0, grid=grid, in_specs=in_specs, out_specs=out_specs, scratch_shapes=scratch),
        out_shape=out_shape,
        compiler_params=pltpu.CompilerParams(dimension_semantics=("arbitrary",) * len(grid), vmem_limit_bytes=VMEM, **more),
        cost_estimate=pl.CostEstimate(flops=int(flops), transcendentals=0, bytes_accessed=int(read)),
    )


def _kept(shape):
    return pl.BlockSpec(shape, lambda *_: (0,) * len(shape), pipeline_mode=pl.Buffered(1))


def normed(h):
    wide = h.astype(F32)
    scale = lax.rsqrt(jnp.mean(wide**2, -1, keepdims=True) + 1e-6)
    return (wide * scale).astype(BF)


def tables(tokens):
    half = HEAD // 2
    angle = jnp.arange(tokens, dtype=F32)[:, None] * THETA ** (-jnp.arange(half, dtype=F32) / half)
    cos, sin = jnp.cos(angle), jnp.sin(angle)
    return jnp.concatenate([cos, cos], -1), jnp.concatenate([-sin, sin], -1)


def _turn(t, cos, sin):
    wide = t.astype(F32)
    return (wide * cos + pltpu.roll(wide, HEAD // 2, 1) * sin).astype(BF)


def _qkv_kernel(h_ref, wq_ref, wk_ref, wv_ref, cos_ref, sin_ref, a_ref, q_ref, k_ref, v_ref):
    a = normed(h_ref[...])
    a_ref[...] = a
    cos, sin = cos_ref[...], sin_ref[...]
    for w_ref, o_ref, turns in ((wq_ref, q_ref, True), (wk_ref, k_ref, True), (wv_ref, v_ref, False)):
        for n in range(0, o_ref.shape[1], 512):
            t = _dot(a, w_ref[0, :, n : n + 512], 1, 0).astype(BF)
            for at in range(0, 512, HEAD):
                one = t[:, at : at + HEAD]
                o_ref[:, n + at : n + at + HEAD] = _turn(one, cos, sin) if turns else one


def qkv(h, wq, wk, wv, cos, sin, number):
    tokens, d = h.shape
    wide = wq.shape[2]
    bt = 256
    rows = lambda n: pl.BlockSpec((bt, n), lambda i: (i, 0))
    weight = pl.BlockSpec((1, d, wide), lambda i: (number, 0, 0), pipeline_mode=pl.Buffered(1))
    return _call(_qkv_kernel, (tokens // bt,), [rows(d), weight, weight, weight, rows(HEAD), rows(HEAD)], [rows(d)] + [rows(wide)] * 3,
                 [jax.ShapeDtypeStruct((tokens, d), BF)] + [jax.ShapeDtypeStruct((tokens, wide), BF)] * 3, [],
                 6 * tokens * d * wide, 6 * d * wide + 6 * tokens * wide)(h, wq, wk, wv, cos, sin)


def _gap(bk, cols):
    return lax.broadcasted_iota(jnp.int32, (bk, cols), 1) - lax.broadcasted_iota(jnp.int32, (bk, cols), 0)


def _attend_kernel(q_ref, k_ref, v_ref, o_ref, lse_ref, top_s, mix_s, gap_s, *, scale, bq, bk, heads):
    iq = pl.program_id(0)
    e = scale * LOG2E

    @pl.when(iq == 0)
    def _():
        gap_s[...] = _gap(bq, bq)

    top_s[...] = jnp.full(top_s.shape, NEG, F32)
    mix_s[...] = jnp.zeros(mix_s.shape, F32)
    ones = jnp.ones((8, bk), BF)
    cut = [slice(i * HEAD, (i + 1) * HEAD) for i in range(heads)]

    def block(start, size, masked):
        here = pl.ds(pl.multiple_of(start, size), size)
        scores = [_dot(k_ref[here, c], q_ref[:, c], 1, 1) for c in cut]
        ok = gap_s[...] >= 0 if masked else None
        weights, keeps = [], []
        for i, s in enumerate(scores):
            if masked:
                s = jnp.where(ok, s, HIDDEN)
            old = top_s[i : i + 1, :]
            top = jnp.maximum(old, s.max(axis=0, keepdims=True))
            top_s[i : i + 1, :] = top
            weights.append(jnp.exp2((s - top) * e).astype(BF))
            keeps.append(jnp.exp2((old - top) * e))
        for i, (p, keep) in enumerate(zip(weights, keeps)):
            values = jnp.concatenate([v_ref[here, cut[i]].T, ones[:, :size]], axis=0)
            mix_s[i] = mix_s[i] * keep + _dot(values, p, 1, 0)

    whole = lax.div(iq * bq, bk)
    lax.fori_loop(0, whole, lambda j, _: block(j * bk, bk, False), None)

    @pl.when(lax.rem(iq, 2) == 1)
    def _():
        block((iq - 1) * bq, bq, False)

    block(iq * bq, bq, True)
    for i in range(heads):
        top, total = top_s[i : i + 1, :], mix_s[i, HEAD : HEAD + 1, :]
        o_ref[:, cut[i]] = (mix_s[i, :HEAD, :] * (1 / total)).T.astype(BF)
        lse_ref[i : i + 1, :] = top * scale + jnp.log(total)


def attend(q, k, v):
    tokens, wide = q.shape
    heads = wide // HEAD
    bq, bk = 256, 512
    rows = pl.BlockSpec((bq, wide), lambda i: (i, 0))
    kernel = functools.partial(_attend_kernel, scale=HEAD**-0.5, bq=bq, bk=bk, heads=heads)
    return _call(kernel, (tokens // bq,), [rows, _kept((tokens, wide)), _kept((tokens, wide))],
                 [rows, pl.BlockSpec((heads, bq), lambda i: (0, i))],
                 [jax.ShapeDtypeStruct((tokens, wide), BF), jax.ShapeDtypeStruct((heads, tokens), F32)],
                 [pltpu.VMEM((heads, bq), F32), pltpu.VMEM((heads, HEAD + 8, bq), F32), pltpu.VMEM((bq, bq), jnp.int32)],
                 4 * tokens * tokens * wide, 8 * tokens * wide)(q, k, v)


def _attend_bwd_kernel(q_ref, k_ref, v_ref, do_ref, o_ref, lse_ref, cos_ref, sin_ref, dq_ref, dk_ref, dv_ref, dq_s, dk_s, dv_s, gap_s,
                       *, scale, bq, bk, heads):
    iq = pl.program_id(1)
    e = scale * LOG2E
    cut = [slice(i * HEAD, (i + 1) * HEAD) for i in range(heads)]

    @pl.when(iq == 0)
    def _():
        gap_s[...] = _gap(bq // 2, bq)
        dk_s[...] = jnp.zeros_like(dk_s)
        dv_s[...] = jnp.zeros_like(dv_s)

    dq_s[...] = jnp.zeros_like(dq_s)
    lses = [lse_ref[0, i : i + 1, :] * LOG2E for i in range(heads)]
    row = jnp.ones((8, HEAD), BF)
    deltas = []
    for c in cut:
        both = do_ref[:, c].astype(F32) * o_ref[:, c].astype(F32)
        high = both.astype(BF)
        low = (both - high.astype(F32)).astype(BF)
        deltas.append((_dot(row, high, 1, 1) + _dot(row, low, 1, 1))[:1, :])

    def block(start, size, first, masked):
        here = pl.ds(pl.multiple_of(start, size), size)
        qs, dos = [q_ref[first:, c] for c in cut], [do_ref[first:, c] for c in cut]
        scores = [_dot(k_ref[here, c], x, 1, 1) for c, x in zip(cut, qs)]
        dps = [_dot(v_ref[here, c], x, 1, 1) for c, x in zip(cut, dos)]
        ok = gap_s[:size, : bq - first] >= 0 if masked else None
        for i, c in enumerate(cut):
            p = jnp.exp2(scores[i] * e - lses[i][:, first:])
            if masked:
                p = jnp.where(ok, p, 0.0)
            ds = (p * (dps[i] - deltas[i][:, first:])).astype(BF)
            dv_s[i, here, :] += _dot(p.astype(BF), dos[i], 1, 0)
            dk_s[i, here, :] += _dot(ds, qs[i], 1, 0)
            dq_s[i, :, first:] += _dot(k_ref[here, c].T, ds, 1, 0)

    half = bq // 2
    lax.fori_loop(0, iq, lambda j, _: block(j * bk, bk, 0, False), None)
    block(iq * bq, half, 0, True)
    block(iq * bq + half, half, half, True)
    here = pl.ds(pl.multiple_of(iq * bq, bq), bq)
    for i, c in enumerate(cut):
        dq_ref[:, c] = _turn((dq_s[i] * scale).T.astype(BF), cos_ref[here, :], -sin_ref[here, :])

    @pl.when(iq == pl.num_programs(1) - 1)
    def _():
        for i, c in enumerate(cut):
            dk_ref[:, c] = _turn((dk_s[i] * scale).astype(BF), cos_ref[...], -sin_ref[...])
            dv_ref[:, c] = dv_s[i].astype(BF)


def attend_bwd(q, k, v, do, o, lse, cos, sin):
    tokens, wide = q.shape
    heads = 4
    groups = wide // HEAD // heads
    bq, bk = 512, 512
    rows = pl.BlockSpec((bq, heads * HEAD), lambda g, i: (i, g))
    keys = pl.BlockSpec((tokens, heads * HEAD), lambda g, i: (0, g))
    kernel = functools.partial(_attend_bwd_kernel, scale=HEAD**-0.5, bq=bq, bk=bk, heads=heads)
    return _call(kernel, (groups, tokens // bq),
                 [rows, keys, keys, rows, rows, pl.BlockSpec((1, heads, bq), lambda g, i: (g, 0, i)), _kept((tokens, HEAD)), _kept((tokens, HEAD))],
                 [rows, keys, keys], [jax.ShapeDtypeStruct((tokens, wide), BF)] * 3,
                 [pltpu.VMEM((heads, HEAD, bq), F32), pltpu.VMEM((heads, tokens, HEAD), F32), pltpu.VMEM((heads, tokens, HEAD), F32),
                  pltpu.VMEM((bq // 2, bq), jnp.int32)],
                 10 * tokens * tokens * wide, 16 * tokens * wide)(q, k, v, do, o, lse.reshape(groups, heads, tokens), cos, sin)


def _sigmoid(x):
    return 0.5 * jnp.tanh(0.5 * x) + 0.5


def _mlp_kernel(b_ref, h_ref, wg_ref, wu_ref, wd_ref, out_ref, acc_s, *, bt):
    j = pl.program_id(0)

    @pl.when(j == 0)
    def _():
        acc_s[...] = jnp.zeros_like(acc_s)

    for at in range(0, b_ref.shape[0], bt):
        b = b_ref[at : at + bt, :]
        gate, up = _dot(b, wg_ref[0], 1, 0), _dot(b, wu_ref[0], 1, 0)
        act = (gate * _sigmoid(gate) * up).astype(BF)
        acc_s[at : at + bt, :] += _dot(act, wd_ref[0], 1, 0)

    @pl.when(j == pl.num_programs(0) - 1)
    def _():
        out_ref[...] = h_ref[...] + acc_s[...].astype(BF)


def mlp(b, h, wg, wu, wd, number):
    tokens, d = b.shape
    ff = wg.shape[2]
    bf = 512
    across = pl.BlockSpec((1, d, bf), lambda j: (number, 0, j))
    down = pl.BlockSpec((1, bf, d), lambda j: (number, j, 0))
    whole = _kept((tokens, d))
    return _call(functools.partial(_mlp_kernel, bt=512), (ff // bf,), [whole, whole, across, across, down], whole,
                 jax.ShapeDtypeStruct((tokens, d), BF), [pltpu.VMEM((tokens, d), F32)],
                 6 * tokens * d * ff, 6 * d * ff)(b, h, wg, wu, wd)


def _mlp_bwd_kernel(b_ref, do_ref, wg_ref, wu_ref, wd_ref, db_ref, dw_ref, bt_s, dot_s, act_s, dg_s, du_s, dbt_s, stage, sems, *, bt):
    j, blocks = pl.program_id(0), pl.num_programs(0)
    tokens, _ = b_ref.shape
    slot = lax.rem(j, 2)

    @pl.when(j == 0)
    def _():
        for at in range(0, tokens, bt):
            bt_s[:, at : at + bt] = b_ref[at : at + bt, :].T
            dot_s[:, at : at + bt] = do_ref[at : at + bt, :].T
        dbt_s[...] = jnp.zeros_like(dbt_s)

    def copies(j, slot):
        targets = (dw_ref.at[:, j], dw_ref.at[:, blocks + j], dw_ref.at[j, pl.ds(2 * blocks, blocks)])
        return [pltpu.make_async_copy(stage.at[slot, n], to, sems.at[slot, n]) for n, to in enumerate(targets)]

    @pl.when(j >= 2)
    def _():
        for copy in copies(j - 2, slot):
            copy.wait()

    wg, wu, wd = wg_ref[0], wu_ref[0], wd_ref[0]
    wgt, wut = wg.T, wu.T
    for at in range(0, tokens, bt):
        b = bt_s[:, at : at + bt]
        gate, up = _dot(wgt, b, 1, 0), _dot(wut, b, 1, 0)
        da = _dot(wd, dot_s[:, at : at + bt], 1, 0).astype(BF).astype(F32)
        s = _sigmoid(gate)
        silu = gate * s
        act_s[:, at : at + bt] = (silu * up).astype(BF)
        du = (da * silu).astype(BF)
        dg = (da * up * (s + silu * (1 - s))).astype(BF)
        du_s[:, at : at + bt] = du
        dg_s[:, at : at + bt] = dg
        dbt_s[:, at : at + bt] += _dot(wg, dg, 1, 0) + _dot(wu, du, 1, 0)
    b, do = b_ref[...], do_ref[...]
    shape = stage.shape[2:]
    stage[slot, 0] = _dot(dg_s[...], b, 1, 0).astype(BF).T.reshape(shape)
    stage[slot, 1] = _dot(du_s[...], b, 1, 0).astype(BF).T.reshape(shape)
    stage[slot, 2] = _dot(act_s[...], do, 1, 0).astype(BF).reshape(shape)
    for copy in copies(j, slot):
        copy.start()

    @pl.when(j == blocks - 1)
    def _():
        for at in range(0, tokens, bt):
            db_ref[at : at + bt, :] = dbt_s[:, at : at + bt].T.astype(BF)
        for copy in copies(j - 1, 1 - slot):
            copy.wait()
        for copy in copies(j, slot):
            copy.wait()


def mlp_bwd(b, do, wg, wu, wd, number, parts):
    tokens, d = b.shape
    ff = wg.shape[2]
    bf = ff // parts
    rows = d // parts
    across = pl.BlockSpec((1, d, bf), lambda j: (number, 0, j))
    down = pl.BlockSpec((1, bf, d), lambda j: (number, j, 0))
    whole = _kept((tokens, d))
    return _call(functools.partial(_mlp_bwd_kernel, bt=512), (parts,), [whole, whole, across, across, down],
                 [whole, pl.BlockSpec(memory_space=pl.ANY)],
                 [jax.ShapeDtypeStruct((tokens, d), BF), jax.ShapeDtypeStruct((parts, 3 * parts, rows, d), BF)],
                 [pltpu.VMEM((d, tokens), BF), pltpu.VMEM((d, tokens), BF)] + [pltpu.VMEM((bf, tokens), BF)] * 3
                 + [pltpu.VMEM((d, tokens), F32), pltpu.VMEM((2, 3, parts, rows, d), BF), pltpu.SemaphoreType.DMA((2, 3))],
                 16 * tokens * d * ff, 12 * d * ff)(b, do, wg, wu, wd)


def _project_bwd_kernel(a_ref, dq_ref, dk_ref, dv_ref, wq_ref, wk_ref, wv_ref, dwo_ref, dw_ref, da_ref, at_s, da_s, *, per, onward):
    n = pl.program_id(0)
    tokens = a_ref.shape[0]

    @pl.when(n == 0)
    def _():
        for at in range(0, tokens, 512):
            at_s[:, at : at + 512] = a_ref[at : at + 512, :].T
        if onward:
            da_s[...] = jnp.zeros_like(da_s)

    for which, (g_ref, w_ref) in enumerate(((dq_ref, wq_ref), (dk_ref, wk_ref), (dv_ref, wv_ref))):
        @pl.when((n >= which * per) & (n < (which + 1) * per))
        def _(g_ref=g_ref, w_ref=w_ref):
            dw_ref[...] = _dot(at_s[...], g_ref[...], 1, 0).astype(BF).reshape(dw_ref.shape)
            if onward:
                for at in range(0, tokens, 512):
                    da_s[at : at + 512, :] += _dot(g_ref[at : at + 512, :], w_ref[0], 1, 1)

    @pl.when(n >= 3 * per)
    def _():
        dw_ref[...] = dwo_ref[...]

    @pl.when(n == pl.num_programs(0) - 1)
    def _():
        da_ref[...] = da_s[...].astype(BF) if onward else jnp.zeros_like(da_ref)


def project_bwd(a, dq, dk, dv, wq, wk, wv, dwo, number, parts, onward):
    tokens, d = a.shape
    wide = dq.shape[1]
    bc = 512
    per, rows = wide // bc, d // parts
    steps = 4 * per
    block = lambda which: lambda n: (0, jnp.clip(n - which * per, 0, per - 1))
    weight = lambda which: lambda n: (number, 0, jnp.clip(n - which * per, 0, per - 1))
    out_rows = (tokens, d) if onward else (8, d)
    return _call(functools.partial(_project_bwd_kernel, per=per, onward=onward), (steps,),
                 [_kept((tokens, d))] + [pl.BlockSpec((tokens, bc), block(i)) for i in range(3)] + [pl.BlockSpec((1, d, bc), weight(i)) for i in range(3)]
                 + [pl.BlockSpec((parts, 1, rows, d), lambda n: (0, jnp.clip(n - 3 * per, 0, per - 1), 0, 0))],
                 [pl.BlockSpec((parts, 1, rows, bc), lambda n: (0, n, 0, 0)), _kept(out_rows)],
                 [jax.ShapeDtypeStruct((parts, steps, rows, bc), BF), jax.ShapeDtypeStruct(out_rows, BF)],
                 [pltpu.VMEM((d, tokens), BF), pltpu.VMEM(out_rows, F32)],
                 (12 if onward else 6) * tokens * d * wide, 12 * tokens * wide)(
                     a, dq, dk, dv, wq, wk, wv, dwo.reshape(parts, per, rows, d))


def _total_kernel(x_ref, o_ref, slots, send, recv, *, n):
    me = lax.axis_index("dp")
    barrier = pltpu.get_barrier_semaphore()
    for k in range(1, n):
        pl.semaphore_signal(barrier, inc=1, device_id={"dp": lax.rem(me + k, n)}, device_id_type=pl.DeviceIdType.MESH)
    pl.semaphore_wait(barrier, n - 1)
    copies = []
    for k in range(1, n):
        copy = pltpu.make_async_remote_copy(src_ref=x_ref, dst_ref=slots.at[me], send_sem=send.at[k], recv_sem=recv.at[k],
                                            device_id={"dp": lax.rem(me + k, n)}, device_id_type=pl.DeviceIdType.MESH)
        copy.start()
        copies.append(copy)
    slots[me] = x_ref[...]
    for copy in copies:
        copy.wait()
    total = slots[0]
    for k in range(1, n):
        total = total + slots[k]
    o_ref[...] = total


def total(x, n):
    wide = jnp.broadcast_to(x, (8, 128))
    spec = pl.BlockSpec(memory_space=pltpu.VMEM)
    return pl.pallas_call(
        functools.partial(_total_kernel, n=n),
        out_shape=jax.ShapeDtypeStruct((8, 128), F32), in_specs=[spec], out_specs=spec,
        scratch_shapes=[pltpu.VMEM((n, 8, 128), F32), pltpu.SemaphoreType.DMA((n,)), pltpu.SemaphoreType.DMA((n,))],
        compiler_params=pltpu.CompilerParams(collective_id=0, has_side_effects=True), name="total",
    )(wide)[0, 0]


def matmul(a, w):
    return jnp.dot(a, w, preferred_element_type=F32).astype(BF)


def adamw(w, m, v, g):
    m = 0.9 * m + 0.1 * g
    v = 0.95 * v + 0.05 * g * g
    step = m * lax.rsqrt(v + 1e-8) + 0.1 * w
    return (w - 0.02 * step).astype(BF), m, v


def side_by_side(t):
    return t.transpose(1, 0, 2).reshape(t.shape[1], -1)


def solution(mesh):
    parts = mesh.shape["dp"]

    def work(x, dy, *arrays):
        weights, m, v = (arrays[i : i + 7] for i in (0, 7, 14))
        wq, wk, wv, wo, wg, wu, wd = weights
        layers, tokens = wq.shape[0], x.shape[1]
        cos, sin = tables(tokens)
        h, kept = x[0], []
        for n in range(layers):
            a, q, k, value = qkv(h, wq, wk, wv, cos, sin, n)
            o, lse = attend(q, k, value)
            mid = h + matmul(o, wo[n])
            b = normed(mid)
            kept.append((h, a, q, k, value, o, lse, mid, b))
            if n < layers - 1:
                h = mlp(b, mid, wg, wu, wd, n)
        by_h, sums = dy[0], [None] * layers
        for n in reversed(range(layers)):
            h, a, q, k, value, o, lse, mid, b = kept[n]
            by_b, dw = mlp_bwd(b, by_h, wg, wu, wd, n, parts)
            hidden = lax.psum_scatter(dw.reshape(parts, -1, dw.shape[-1]), "dp", scatter_dimension=0, tiled=True)[0]
            by_mid = by_h + jax.vjp(normed, mid)[1](by_b)[0]
            by_o, dwo = matmul(by_mid, wo[n].T), matmul(o.T, by_mid)
            dq, dk, dv = attend_bwd(q, k, value, by_o, o, lse, cos, sin)
            dw, by_a = project_bwd(a, dq, dk, dv, wq, wk, wv, dwo, n, parts, n > 0)
            heads = lax.psum_scatter(dw.reshape(parts, -1, dw.shape[-1]), "dp", scatter_dimension=0, tiled=True)[0]
            if n > 0:
                by_h = by_mid + jax.vjp(normed, h)[1](by_a)[0]
            sums[n] = hidden, heads
        everything = [t for pair in sums for t in pair]
        squares = total(sum(jnp.sum(t.astype(F32) ** 2) for t in everything), parts)
        factor = jnp.minimum(1.0, 0.5 * lax.rsqrt(squares / (parts * sum(t.size for t in everything)) + 1e-30))
        me = lax.axis_index("dp")
        new = [None] * 7

        def update(some, gradients):
            for i, g in zip(some, gradients, strict=True):
                own = lax.dynamic_slice_in_dim(weights[i], me * m[i].shape[1], m[i].shape[1], 1).astype(F32)
                new[i] = adamw(own, m[i], v[i], jnp.stack(g).astype(F32) * factor)
            return joined([new[i][0] for i in some])

        rows = x.shape[2] // parts
        flat = update(HIDDEN_LAYER, zip(*(split(pair[0], rows, parts, 2) for pair in sums)))
        flat, others = lax.optimization_barrier((flat, [pair[1] for pair in sums]))
        per = others[0].shape[0] // rows // 4
        whole = [None] * 7
        every = gather(flat)
        others = update(HEADS, zip(*(split(t, rows, per, 3) for t in others)))
        others = gather(others)
        for some, array, several in ((HIDDEN_LAYER, every, 1), (HEADS, others, 4)):
            for i, one in zip(some, spread(array, [weights[i].shape for i in some], several), strict=True):
                whole[i] = one
        return (*whole, *(one[1] for one in new), *(one[2] for one in new))

    states, all_of, cut = P(("rep", "dp"), None, None), P(None, None, None), P(None, "dp", None)
    return jax.shard_map(
        work,
        mesh=mesh,
        in_specs=(states, states) + (all_of,) * 7 + (cut,) * 14,
        out_specs=(P("rep", None, None),) * 7 + (P("rep", "dp", None),) * 14,
        check_vma=False,
    )


def _spread_kernel(*refs):
    count = len(refs) // 2
    for from_ref, to_ref in zip(refs[:count], refs[count:]):
        devices, _, rows, _ = from_ref.shape
        _, together, columns = to_ref.shape
        own = together // devices
        for n in range(devices):
            for at in range(0, own, rows):
                left = at // rows * columns
                to_ref[0, n * own + at : n * own + at + rows, :] = from_ref[n, 0, :, left : left + columns]


def spread(every, shapes, several):
    parts, slots, rows, columns = every.shape
    layers = slots // len(shapes)
    source = lambda at: pl.BlockSpec((several, 1, rows, columns), lambda n, i: (i, at * layers + n, 0, 0))
    target = lambda shape: pl.BlockSpec((1, several * shape[1] // parts, shape[2]), lambda n, i: (n, i, 0))
    return _call(_spread_kernel, (layers, parts // several), [source(at) for at in range(len(shapes))], [target(shape) for shape in shapes],
                 [jax.ShapeDtypeStruct(shape, BF) for shape in shapes], [], every.size, 4 * every.size)(*[every] * len(shapes))


HEADS, HIDDEN_LAYER = (0, 1, 2, 3), (4, 5, 6)


def joined(own):
    shape = own[0].shape
    return jnp.concatenate([t.reshape(shape[0], -1, shape[1], t.shape[2]).transpose(0, 2, 1, 3).reshape(shape) for t in own], 0)


def gather(flat):
    return lax.all_gather(flat, "dp", axis=0)


def split(t, rows, per, count):
    t = t.reshape(-1, rows, t.shape[-1])
    return [side_by_side(t[i * per : (i + 1) * per]) for i in range(count)] + [t[count * per :].reshape(-1, t.shape[-1])]
```
